16 devices in a mesh: dp: 2 (over y, z), cp: 8 (over x, core).
Axes of the slice: x: 4, y: 2, z: 1, core: 2. Of those that a mesh axis runs over, the one named last changes fastest.
The devices are a block of a 4x4x8 slice.
Arguments:
- queries: bfloat16 [2, 4096, 16, 256], P('dp', 'cp'), parts along dimension 0
- keys: bfloat16 [2, 4096, 8, 256], P('dp', 'cp'), parts along dimension 0
- values: bfloat16 [2, 4096, 8, 256], P('dp', 'cp'), parts along dimension 0
- out_grad: bfloat16 [2, 4096, 16, 256], P('dp', 'cp'), parts along dimension 0
Outputs:
- output 1: bfloat16 [2, 4096, 16, 256], P('dp', 'cp'), parts along dimension 0
- output 2: float32 [2, 16, 4096], P('dp', None, 'cp'), parts along dimension 0
- output 3: bfloat16 [2, 4096, 16, 256], P('dp', 'cp'), parts along dimension 0
- output 4: bfloat16 [2, 4096, 8, 256], P('dp', 'cp'), parts along dimension 0
- output 5: bfloat16 [2, 4096, 8, 256], P('dp', 'cp'), parts along dimension 0
There are 2 independent parts. The reference program is written for one: setup_inputs(seed, part) draws one part's arguments, and reference() takes and returns one part's arrays. A program takes and returns all parts, laid end to end along the dimension named above; each array names one.
All inputs are finite; a program needn't handle non-finite values.
Results may differ from the reference program's by a relative error of at most 0.0187391.
Values are sent between devices in bfloat16 or wider.
A program may use at most 768 MiB of HBM per device.

```python
import jax
import jax.numpy as jnp
from jax import lax

BATCH = 1
SEQ = 4096
HEADS = 16
KV_HEADS = 8
HEAD = 256
QBLOCK = 128

RATIO = HEADS // KV_HEADS
SCALE = HEAD ** -0.5
NUM_BLOCKS = SEQ // QBLOCK


def setup_inputs(seed: int = 0, part: int = 0) -> dict:
    base_key = jax.random.fold_in(jax.random.key(seed), part)
    rng_keys = jax.random.split(base_key, 4)
    q_shape = (BATCH, SEQ, HEADS, HEAD)
    kv_shape = (BATCH, SEQ, KV_HEADS, HEAD)
    queries = jax.random.normal(rng_keys[0], q_shape, jnp.float32).astype(jnp.bfloat16)
    keys = jax.random.normal(rng_keys[1], kv_shape, jnp.float32).astype(jnp.bfloat16)
    values = jax.random.normal(rng_keys[2], kv_shape, jnp.float32).astype(jnp.bfloat16)
    out_grad = jax.random.normal(rng_keys[3], q_shape, jnp.float32).astype(jnp.bfloat16)
    return {"queries": queries, "keys": keys, "values": values, "out_grad": out_grad}


def reference(queries, keys, values, out_grad):
    keys_f = keys.astype(jnp.float32)
    values_f = values.astype(jnp.float32)
    key_pos = jnp.arange(SEQ)
    query_blocks = jnp.moveaxis(queries.reshape(BATCH, NUM_BLOCKS, QBLOCK, KV_HEADS, RATIO, HEAD), 1, 0)
    grad_blocks = jnp.moveaxis(out_grad.reshape(BATCH, NUM_BLOCKS, QBLOCK, KV_HEADS, RATIO, HEAD), 1, 0)

    def block_step(carry, block_in):
        grad_key, grad_value = carry
        block_idx, query_blk, grad_blk = block_in
        query_f = query_blk.astype(jnp.float32)
        grad_f = grad_blk.astype(jnp.float32)
        query_pos = block_idx * QBLOCK + jnp.arange(QBLOCK)
        causal = query_pos[:, None] >= key_pos[None, :]
        scores = jnp.einsum("bqgrd,bkgd->bgrqk", query_f, keys_f) * SCALE
        scores = jnp.where(causal, scores, -jnp.inf)
        row_max = jnp.max(scores, axis=-1, keepdims=True)
        row_lse = row_max + jnp.log(jnp.sum(jnp.exp(scores - row_max), axis=-1, keepdims=True))
        prob_mat = jnp.exp(scores - row_lse)
        prob_round = prob_mat.astype(jnp.bfloat16).astype(jnp.float32)
        out_blk = jnp.einsum("bgrqk,bkgd->bqgrd", prob_round, values_f).astype(jnp.bfloat16)
        delta = jnp.einsum("bqgrd,bqgrd->bgrq", grad_f, out_blk.astype(jnp.float32))
        grad_prob = jnp.einsum("bqgrd,bkgd->bgrqk", grad_f, values_f)
        grad_score = prob_mat * (grad_prob - delta[..., None])
        score_round = grad_score.astype(jnp.bfloat16).astype(jnp.float32)
        grad_query = jnp.einsum("bgrqk,bkgd->bqgrd", score_round, keys_f) * SCALE
        grad_key = grad_key + jnp.einsum("bgrqk,bqgrd->bkgd", score_round, query_f) * SCALE
        grad_value = grad_value + jnp.einsum("bgrqk,bqgrd->bkgd", prob_round, grad_f)
        return (grad_key, grad_value), (out_blk, row_lse[..., 0], grad_query.astype(jnp.bfloat16))

    zero_kv = jnp.zeros((BATCH, SEQ, KV_HEADS, HEAD), jnp.float32)
    carry_out, block_outs = lax.scan(block_step, (zero_kv, zero_kv), (jnp.arange(NUM_BLOCKS), query_blocks, grad_blocks))
    out_blocks, lse_blocks, dq_blocks = block_outs
    attn_out = jnp.moveaxis(out_blocks, 0, 1).reshape(BATCH, SEQ, HEADS, HEAD)
    row_lse = jnp.moveaxis(lse_blocks, 0, 3).reshape(BATCH, HEADS, SEQ)
    grad_query = jnp.moveaxis(dq_blocks, 0, 1).reshape(BATCH, SEQ, HEADS, HEAD)
    grad_key = carry_out[0].astype(jnp.bfloat16)
    grad_value = carry_out[1].astype(jnp.bfloat16)
    return attn_out, row_lse, grad_query, grad_key, grad_value
```

```python
import functools

import jax
import jax.numpy as jnp
from jax import lax
from jax.experimental import pallas as pl
from jax.experimental.pallas import tpu as pltpu
from jax.sharding import PartitionSpec as P

MESH = pl.DeviceIdType.MESH
F32 = jnp.float32
BF16 = jnp.bfloat16


def dot_nt(lhs, rhs):
    return lax.dot_general(lhs, rhs, (((1,), (1,)), ((), ())), preferred_element_type=F32)


def dot_nn(lhs, rhs):
    return lax.dot_general(lhs, rhs, (((1,), (0,)), ((), ())), preferred_element_type=F32)


def attention_kernel(n, ratio, scale,
                     q_in, k_in, v_in, g_in,
                     o_out, l_out, dq_out, dk_out, dv_out,
                     q_all, k_all, v_all, g_all, kt_all, vt_all,
                     o_send, l_send, dq_send, dk_send, dv_send,
                     d_row, acc, dk_acc, dv_acc,
                     in_send, in_recv, out_send, out_recv, own_sem):
    me = lax.axis_index("cp")
    tokens = k_in.shape[1]
    cols = ratio * tokens

    def peer(shift):
        return lax.rem(me + shift + n, n)

    barrier = pltpu.get_barrier_semaphore()
    for shift in range(1, n):
        pl.semaphore_signal(barrier, inc=1, device_id={"cp": peer(shift)}, device_id_type=MESH)
    pl.semaphore_wait(barrier, n - 1)

    arrivals = ((k_in, k_all), (v_in, v_all), (q_in, q_all), (g_in, g_all))

    def in_copy(which, dest, source):
        src, dst = arrivals[which]
        return pltpu.make_async_remote_copy(
            src_ref=src.at[dest], dst_ref=dst.at[source],
            send_sem=in_send.at[which, dest], recv_sem=in_recv.at[which, source],
            device_id={"cp": dest}, device_id_type=MESH)

    def own_copy(which):
        src, dst = arrivals[which]
        return pltpu.make_async_copy(src.at[me], dst.at[me], own_sem.at[which])

    for which in range(4):
        own_copy(which).start()
        for shift in range(1, n):
            in_copy(which, peer(-shift), me).start()

    departures = ((o_send, o_out), (l_send, l_out), (dq_send, dq_out), (dk_send, dk_out), (dv_send, dv_out))

    def out_copy(which, dest, source):
        src, dst = departures[which]
        return pltpu.make_async_remote_copy(
            src_ref=src.at[dest], dst_ref=dst.at[source],
            send_sem=out_send.at[which, dest], recv_sem=out_recv.at[which, source],
            device_id={"cp": dest}, device_id_type=MESH)

    def home_copy(which):
        src, dst = departures[which]
        return pltpu.make_async_copy(src.at[me], dst.at[me], own_sem.at[4 + which])

    def ship(which, shift, dest):
        @pl.when(shift == 0)
        def _():
            home_copy(which).start()

        @pl.when(shift != 0)
        def _():
            out_copy(which, dest, me).start()

    def arrive(which, shift, source):
        @pl.when(shift == 0)
        def _():
            own_copy(which).wait()

        @pl.when(shift != 0)
        def _():
            in_copy(which, source, source).wait_recv()

    def prepare(shift, carry):
        source = peer(shift)
        arrive(0, shift, source)
        kt_all[source] = k_all[source].T
        arrive(1, shift, source)
        vt_all[source] = v_all[source].T
        dk_acc[source] = jnp.zeros(dk_acc.shape[1:], F32)
        dv_acc[source] = jnp.zeros(dv_acc.shape[1:], F32)
        return carry

    lax.fori_loop(0, n, prepare, 0)

    def scores(i, j, causal):
        out = dot_nt(k_all[j], q_all[i]) * scale
        if causal:
            key_idx = lax.broadcasted_iota(jnp.int32, out.shape, 0)
            query_idx = lax.rem(lax.broadcasted_iota(jnp.int32, out.shape, 1), tokens)
            out = jnp.where(key_idx <= query_idx, out, -jnp.inf)
        return out

    def forward_row(shift, carry):
        i = peer(shift)
        arrive(2, shift, i)
        first = scores(i, i, True)
        row_max = jnp.max(first, axis=0, keepdims=True)
        weights = jnp.exp(first - row_max)
        row_sum = jnp.sum(weights, axis=0, keepdims=True)
        acc[...] = dot_nn(vt_all[i], weights.astype(BF16))

        def visit(j, state):
            run_max, run_sum = state
            block = scores(i, j, False)
            new_max = jnp.maximum(run_max, jnp.max(block, axis=0, keepdims=True))
            alpha = jnp.exp(run_max - new_max)
            weights = jnp.exp(block - new_max)
            acc[...] = acc[...] * alpha + dot_nn(vt_all[j], weights.astype(BF16))
            return new_max, run_sum * alpha + jnp.sum(weights, axis=0, keepdims=True)

        row_max, row_sum = lax.fori_loop(0, i, visit, (row_max, row_sum))
        o_send[i] = (acc[...] / row_sum).T.astype(BF16)
        l_send[i] = row_max + jnp.log(row_sum)
        ship(0, shift, i)
        ship(1, shift, i)
        return carry

    lax.fori_loop(0, n, forward_row, 0)

    def backward_row(shift, carry):
        i = peer(shift)
        arrive(3, shift, i)
        d_row[...] = jnp.sum((g_all[i].astype(F32) * o_send[i].astype(F32)).T, axis=0, keepdims=True)
        acc[...] = jnp.zeros(acc.shape, F32)

        def block_grads(j, causal):
            prob = jnp.exp(scores(i, j, causal) - l_send[i])
            grad_prob = dot_nt(v_all[j], g_all[i])
            grad_score = (prob * (grad_prob - d_row[...])).astype(BF16)
            dv_acc[j] += dot_nn(prob.astype(BF16), g_all[i])
            dk_acc[j] += dot_nn(grad_score, q_all[i])
            acc[...] += dot_nn(kt_all[j], grad_score)

        block_grads(i, True)

        def visit(j, inner):
            block_grads(j, False)
            return inner

        lax.fori_loop(0, i, visit, 0)
        dq_send[i] = (acc[...] * scale).T.astype(BF16)
        ship(2, shift, i)
        return carry

    lax.fori_loop(0, n, backward_row, 0)

    def finish(shift, carry):
        j = peer(shift)
        dk_send[j] = (dk_acc[j] * scale).astype(BF16)
        ship(3, shift, j)
        dv_send[j] = dv_acc[j].astype(BF16)
        ship(4, shift, j)
        return carry

    lax.fori_loop(0, n, finish, 0)

    for which in range(4):
        for shift in range(1, n):
            in_copy(which, peer(-shift), me).wait_send()
    for which in range(5):
        home_copy(which).wait()
        for shift in range(1, n):
            out_copy(which, peer(shift), me).wait_send()
            out_copy(which, peer(-shift), peer(-shift)).wait_recv()


def solution(mesh):
    n = mesh.shape["cp"]

    def attention_shard(queries, keys, values, out_grad):
        batch, tokens, heads, head_dim = queries.shape
        kv_heads = keys.shape[2]
        ratio = heads // kv_heads
        scale = head_dim ** -0.5
        cols = ratio * tokens

        def by_head(array):
            return jnp.transpose(array[0], (1, 0, 2)).reshape(n, -1, head_dim)

        q_shape, kv_shape = (n, cols, head_dim), (n, tokens, head_dim)
        hbm = pl.BlockSpec(memory_space=pl.ANY)
        flops = 7 * 2 * cols * tokens * head_dim * n * (n + 1) // 2
        o_out, l_out, dq_out, dk_out, dv_out = pl.pallas_call(
            functools.partial(attention_kernel, n, ratio, scale),
            out_shape=(
                jax.ShapeDtypeStruct(q_shape, BF16),
                jax.ShapeDtypeStruct((n, 1, cols), F32),
                jax.ShapeDtypeStruct(q_shape, BF16),
                jax.ShapeDtypeStruct(kv_shape, BF16),
                jax.ShapeDtypeStruct(kv_shape, BF16),
            ),
            in_specs=[hbm] * 4,
            out_specs=[hbm] * 5,
            scratch_shapes=[
                pltpu.VMEM(q_shape, BF16),
                pltpu.VMEM(kv_shape, BF16),
                pltpu.VMEM(kv_shape, BF16),
                pltpu.VMEM(q_shape, BF16),
                pltpu.VMEM((n, head_dim, tokens), BF16),
                pltpu.VMEM((n, head_dim, tokens), BF16),
                pltpu.VMEM(q_shape, BF16),
                pltpu.VMEM((n, 1, cols), F32),
                pltpu.VMEM(q_shape, BF16),
                pltpu.VMEM(kv_shape, BF16),
                pltpu.VMEM(kv_shape, BF16),
                pltpu.VMEM((1, cols), F32),
                pltpu.VMEM((head_dim, cols), F32),
                pltpu.VMEM(kv_shape, F32),
                pltpu.VMEM(kv_shape, F32),
                pltpu.SemaphoreType.DMA((4, n)),
                pltpu.SemaphoreType.DMA((4, n)),
                pltpu.SemaphoreType.DMA((5, n)),
                pltpu.SemaphoreType.DMA((5, n)),
                pltpu.SemaphoreType.DMA((9,)),
            ],
            compiler_params=pltpu.CompilerParams(
                collective_id=0, has_side_effects=True, vmem_limit_bytes=67043328
            ),
            cost_estimate=pl.CostEstimate(flops=flops, bytes_accessed=24 * cols * tokens, transcendentals=0),
        )(by_head(queries), by_head(keys), by_head(values), by_head(out_grad))

        def by_token(array, count):
            return jnp.transpose(array.reshape(count, tokens, head_dim), (1, 0, 2))[None]

        return (by_token(o_out, heads), l_out.reshape(batch, heads, tokens), by_token(dq_out, heads),
                by_token(dk_out, kv_heads), by_token(dv_out, kv_heads))

    seq_spec = P("dp", "cp")
    return jax.shard_map(attention_shard, mesh=mesh, in_specs=(seq_spec, seq_spec, seq_spec, seq_spec), out_specs=(seq_spec, P("dp", None, "cp"), seq_spec, seq_spec, seq_spec), check_vma=False)
```
